32 devices in a mesh: grow: 4 (over y, x), gcol: 8 (over z, core).
Axes of the slice: x: 2, y: 2, z: 4, core: 2. Of those that a mesh axis runs over, the one named last changes fastest.
Arguments:
- psi: float32 [32768, 1024], P(('grow', 'gcol')), may hold values from -6 to 6
- vpsi: float32 [32768, 1024], P(('grow', 'gcol')), may hold values from -6 to 6
- kinetic: float32 [32768], P(('grow', 'gcol')), may hold values from 0.1 to 10
- mixing: float32 [1024, 1024], P('grow', 'gcol'), may hold values from -0.1875 to 0.1875
Outputs:
- residual: float32 [32768, 1024], P(('grow', 'gcol'))
- projected: float32 [1024, 1024], P('grow', 'gcol')
The draws below stay inside these ranges and needn't reach their ends.
All inputs are finite; a program needn't handle non-finite values.
Results may differ from the reference program's by a relative error of at most 0.000073.
Values sent between devices are 32-bit elements; how exact they have to be, the bound alone decides.
A program may use at most 128 MiB of HBM per device.

```python
import math
import jax
import jax.numpy as jnp
from jax import lax

NB = 1024
ROWS = 32768


def spiked(result, rng, source, target, blocks, factor):
    owner, partner = [(jnp.arange(result.shape[position]) // (result.shape[position] // blocks)).reshape([-1 if axis == position else 1 for axis in range(result.ndim)]) for position in (source, target)]
    chosen = jax.random.permutation(rng, blocks)[partner]
    strong = (owner == chosen) | (owner == (partner + blocks // 2) % blocks)
    return jnp.where(strong, factor * result, result)


def steps_of(stream_key, shape, split, least, high):
    factor_of = 1.0
    for position, blocks in split:
        steps = jax.random.uniform(jax.random.fold_in(jax.random.fold_in(stream_key, 6), position), (blocks,), jnp.float32, least / len(split), high / len(split))
        factor_of = factor_of * jnp.repeat(jnp.exp(steps), shape[position] // blocks).reshape((-1,) + (1,) * (len(shape) - 1 - position))
    return factor_of


def normal_values(key, shape, spread, reach, shards=(), dtype=jnp.bfloat16):
    values = jax.random.normal(key, shape, jnp.float32) * spread
    if len(shards) > 0:
        values = steps_of(key, shape, shards, -0.22, 0.18) * values
    return jnp.clip(values, min=-reach, max=reach).astype(dtype)


def heavy_noise(own_key, dims, spread, reach, shards, heavy, held_as=jnp.bfloat16):
    values = spread * jax.random.normal(own_key, dims, jnp.float32)
    if shards:
        values = values * steps_of(own_key, dims, shards, -0.22, 0.18)
    return jnp.clip(spiked(values, jax.random.fold_in(own_key, 3), *heavy), -reach, reach).astype(held_as)


def setup_inputs(seed: int = 0) -> dict:
    keys = jax.random.split(jax.random.key(seed), 5)
    psi = normal_values(keys[0], (ROWS, NB), 1.0, 6.0, ((0, 32),), jnp.float32)
    vpsi = heavy_noise(keys[1], (ROWS, NB), 1.0, 6.0, ((0, 32),), (0, 1, 32, 2.75), jnp.float32)
    kinetic = jnp.clip(jnp.exp(math.log(10.0) - 4.6051702 * jax.random.uniform(keys[2], (ROWS,), jnp.float32) ** steps_of(keys[2], (ROWS,), ((0, 32),), -0.2, 0.2)), 0.1, 10.0)
    mixing = normal_values(keys[3], (NB, NB), NB ** -0.5, 0.1875, ((0, 4), (1, 8)), jnp.float32)
    return dict(psi=psi, vpsi=vpsi, kinetic=kinetic, mixing=mixing)


def reference(psi, vpsi, kinetic, mixing):
    hpsi = kinetic[:, None] * psi + vpsi
    projected = lax.dot_general(psi, hpsi, (((0,), (0,)), ((), ())), precision=lax.Precision.HIGHEST, preferred_element_type=jnp.float32) * (1.0 / ROWS)
    correction = hpsi - jnp.dot(psi, projected, precision=lax.Precision.HIGHEST, preferred_element_type=jnp.float32)
    residual = jnp.dot(correction, mixing, precision=lax.Precision.HIGHEST, preferred_element_type=jnp.float32)
    return residual, projected
```

```python
import functools

import jax
import jax.numpy as jnp
from jax import lax
from jax.experimental import pallas as pl
from jax.experimental.pallas import tpu as pltpu
from jax.sharding import PartitionSpec as P

F32 = jnp.float32
BF16 = jnp.bfloat16
TN = 256


def split(x):
    hi = x.astype(BF16)
    return hi, (x - hi.astype(F32)).astype(BF16)


def dot3(ah, al, bh, bl):
    dot = functools.partial(jnp.dot, preferred_element_type=F32)
    return dot(ah, bh) + (dot(ah, bl) + dot(al, bh))


def kernel(nz, scale, psi_hbm, vpsi_hbm, kin_ref, mix_ref, res_ref, proj_ref,
           psi_v, vpsi_v, psh, psl, pth, ptl, hh, hl, mh, ml, part, r0, r1, r2,
           rzr, rzl, mg, q, pown, pin,
           ld, m1s, m1r, m2s, m2r, mzs, mzr, mcs, mcr, mloc,
           s0s, s0r, s1s, s1r, s2s, s2r, zs, zrr, zrl, ps, pr, ploc,
           qzs, qzr, q2s, q2r, q1s, q1r, qcs, qcr):
    rows, nb = psi_v.shape
    n_grow = mg.shape[1]
    n_gcol = mg.shape[0]
    each = part.shape[4]
    bc = nb // n_gcol
    br = nb // n_grow
    half = br // 2
    grp = 2 * half
    g = lax.axis_index("grow")
    gc = lax.axis_index("gcol")
    z = gc // 2
    core = gc % 2
    pc = 1 - core
    w1 = 1 + core
    w2 = 2 - core
    a = (g // w1) % 2
    b = (g // w2) % 2
    ap, bp = b, a
    g1 = g + w1 * (1 - 2 * a)
    g2 = g + w2 * (1 - 2 * b)
    dev_c = {"grow": g, "gcol": z * 2 + pc}
    dev_1 = {"grow": g1, "gcol": gc}
    dev_2 = {"grow": g2, "gcol": gc}
    dev_r = {"grow": g, "gcol": lax.rem(gc + 2, n_gcol)}
    dev_l = {"grow": g, "gcol": lax.rem(gc + n_gcol - 2, n_gcol)}

    def rc(src, dst, ss, rs, dev):
        return pltpu.make_async_remote_copy(
            src_ref=src, dst_ref=dst, send_sem=ss, recv_sem=rs,
            device_id=dev, device_id_type=pl.DeviceIdType.MESH)

    nch = ld.shape[1]
    ch = rows // nch

    def loads(i):
        s = pl.ds(i * ch, ch)
        return (pltpu.make_async_copy(psi_hbm.at[s], psi_v.at[s], ld.at[0, i]),
                pltpu.make_async_copy(vpsi_hbm.at[s], vpsi_v.at[s], ld.at[1, i]))

    for i in range(nch):
        for c in loads(i):
            c.start()
    own_m = pltpu.make_async_copy(mix_ref, mg.at[gc, g], mloc)
    own_m.start()

    barrier = pltpu.get_barrier_semaphore()
    for k in range(1, n_gcol):
        pl.semaphore_signal(barrier, inc=1, device_id={"grow": g, "gcol": lax.rem(gc + k, n_gcol)},
                            device_id_type=pl.DeviceIdType.MESH)
    for dev in (dev_1, dev_2):
        pl.semaphore_signal(barrier, inc=1, device_id=dev, device_id_type=pl.DeviceIdType.MESH)
    pl.semaphore_wait(barrier, n_gcol - 1 + 2)

    m_1 = rc(mix_ref, mg.at[gc, g], m1s, m1r, dev_1)
    m_1.start()

    kt = jnp.transpose(jnp.broadcast_to(kin_ref[...], (128, rows)))
    for i in range(nch):
        for c in loads(i):
            c.wait()
        r = slice(i * ch, (i + 1) * ch)
        for cc in range(2):
            for ba in range(2):
                for bb in range(2):
                    gg = (ba + 2 * bb) if cc == 0 else (2 * ba + bb)
                    for s in range(0, half, 128):
                        col = gg * br + cc * half + s
                        x = psi_v[r, col:col + 128]
                        h = kt[r, :] * x + vpsi_v[r, col:col + 128]
                        hhi, hlo = split(h)
                        hh[r, col:col + 128] = hhi
                        hl[r, col:col + 128] = hlo
                        xhi, xlo = split(x)
                        o = bb * half + s
                        k = cc * 2 + ba
                        psh[k, r, o:o + 128] = xhi
                        psl[k, r, o:o + 128] = xlo
                        pth[k, o:o + 128, r] = jnp.transpose(xhi)
                        ptl[k, o:o + 128, r] = jnp.transpose(xlo)

    own_m.wait()
    m_1.wait()
    mg_1 = [rc(mg.at[gc, gx], mg.at[gc, gx], m2s.at[k], m2r.at[k], dev_2)
            for k, gx in enumerate((g, g1))]
    for c in mg_1:
        c.start()

    def mm1(cx, ax):
        k = cx * 2 + ax

        @pl.loop(0, nb // TN)
        def _(j):
            n = pl.ds(pl.multiple_of(j * TN, TN), TN)
            out = dot3(pth[k], ptl[k], hh[:, n], hl[:, n])
            part[cx, ax, :, :, :, n] = out.reshape(2, nz, each, TN)

    def line(at, ss, rs):
        def right(t):
            return rc(at(z - t), at(z - t), ss.at[0, t], rs.at[z - t], dev_r)

        def left(t):
            return rc(at(z + t), at(z + t), ss.at[1, t], rs.at[z + t], dev_l)

        def step(t):
            @pl.when(z - t >= 0)
            def _():
                if t > 0:
                    rc(at(z - t), at(z - t), ss.at[0, 0], rs.at[z - t], dev_r).wait_recv()

                @pl.when(z < nz - 1)
                def _():
                    if t < nz - 1:
                        right(t).start()

            @pl.when(z + t < nz)
            def _():
                if t > 0:
                    rc(at(z + t), at(z + t), ss.at[1, 0], rs.at[z + t], dev_l).wait_recv()

                @pl.when(z > 0)
                def _():
                    if t < nz - 1:
                        left(t).start()

        def drain():
            for t in range(nz - 1):
                @pl.when((z - t >= 0) & (z < nz - 1))
                def _():
                    right(t).wait_send()

                @pl.when((z + t < nz) & (z > 0))
                def _():
                    left(t).wait_send()

        return step, drain

    m_step, m_drain = line(lambda i: mg.at[2 * i + core], mzs, mzr)

    s0 = []
    for i, ax in enumerate((1 - ap, ap)):
        mm1(pc, ax)
        c = rc(part.at[pc, ax], r0.at[i], s0s.at[i], s0r.at[i], dev_c)
        c.start()
        s0.append(c)
        if i == 0:
            for c in mg_1:
                c.wait()
            m_step(0)

    mm1(core, 1 - a)
    s0[0].wait_recv()
    s1 = []
    for i, bx in enumerate((1 - b, b)):
        part[core, 1 - a, bx] = part[core, 1 - a, bx] + r0[0, bx]
        c = rc(part.at[core, 1 - a, bx], r1.at[i], s1s.at[i], s1r.at[i], dev_1)
        c.start()
        s1.append(c)
    mm1(core, a)
    s0[1].wait_recv()
    for bx in range(2):
        part[core, a, bx] = part[core, a, bx] + r0[1, bx]
    m_step(1)
    s1[0].wait_recv()
    part[core, a, 1 - b] = part[core, a, 1 - b] + r1[0]
    s2 = rc(part.at[core, a, 1 - b], r2, s2s, s2r, dev_2)
    s2.start()
    s1[1].wait_recv()
    part[core, a, b] = part[core, a, b] + r1[1]
    for t in range(2, nz - 1):
        m_step(t)
    s2.wait_recv()
    part[core, a, b] = part[core, a, b] + r2[...]

    def zr(t):
        d = nz - 1 - t
        return rc(part.at[core, a, b, d], rzr.at[d], zs.at[0, t], zrr.at[d], dev_r)

    def zl(t):
        return rc(part.at[core, a, b, t], rzl.at[t], zs.at[1, t], zrl.at[t], dev_l)

    for t in range(nz):
        d = nz - 1 - t

        @pl.when((z > 0) & (d >= z))
        def _():
            rc(part.at[core, a, b, d], rzr.at[d], zs.at[0, 0], zrr.at[d], dev_r).wait_recv()
            part[core, a, b, d] = part[core, a, b, d] + rzr[d]

        if t < nz - 1:
            @pl.when(d > z)
            def _():
                zr(t).start()

        @pl.when((z < nz - 1) & (t <= z))
        def _():
            rc(part.at[core, a, b, t], rzl.at[t], zs.at[1, 0], zrl.at[t], dev_l).wait_recv()
            part[core, a, b, t] = part[core, a, b, t] + rzl[t]

        if t < nz - 1:
            @pl.when(t < z)
            def _():
                zl(t).start()

    own = part[core, a, b, z] * scale
    pown[...] = own
    for k in range(n_gcol):
        pin_k = own[:, k * bc:(k + 1) * bc]
        pin[k] = pin_k
    sends = []
    row0 = pl.multiple_of(core * half + z * each, each)
    for k in range(1, n_gcol):
        to = lax.rem(gc + k, n_gcol)
        c = rc(pin.at[to], proj_ref.at[pl.ds(row0, each)], ps.at[k], pr.at[k],
               {"grow": g, "gcol": to})
        c.start()
        sends.append(c)
    own_p = pltpu.make_async_copy(pin.at[gc], proj_ref.at[pl.ds(row0, each)], ploc)
    own_p.start()

    m_step(nz - 1)
    mc = []
    for i in range(nz):
        c = rc(mg.at[2 * i + core], mg.at[2 * i + core], mcs.at[i], mcr.at[i], dev_c)
        c.start()
        mc.append(c)
    for i in range(nz):
        rc(mg.at[2 * i + pc], mg.at[2 * i + pc], mcs.at[i], mcr.at[i], dev_c).wait_recv()

    @pl.loop(0, n_gcol)
    def _(k):
        n = pl.ds(pl.multiple_of(k * bc, bc), bc)
        for gx in range(n_grow):
            hi, lo = split(mg[k, gx])
            mh[gx * br:(gx + 1) * br, n] = hi
            ml[gx * br:(gx + 1) * br, n] = lo

    ph, plo = split(pown[...])

    @pl.loop(0, nb // TN)
    def _(j):
        n = pl.ds(pl.multiple_of(j * TN, TN), TN)
        q[core, a, b, z, :, n] = dot3(ph, plo, mh[:, n], ml[:, n])

    q_step, q_drain = line(lambda i: q.at[core, a, b, i], qzs, qzr)

    def hmix(i):
        @pl.loop(0, nb // TN)
        def _(j):
            n = pl.ds(pl.multiple_of(j * TN, TN), TN)
            r = slice(i * (rows // 4), (i + 1) * (rows // 4))
            res_ref[r, n] = dot3(hh[r, :], hl[r, :], mh[:, n], ml[:, n])

    def finish(cx, ax):
        k = cx * 2 + ax

        @pl.loop(0, nb // TN)
        def _(j):
            n = pl.ds(pl.multiple_of(j * TN, TN), TN)
            qh, ql = split(q[cx, ax, :, :, :, n].reshape(grp, TN))
            for i in range(4):
                r = slice(i * (rows // 4), (i + 1) * (rows // 4))
                res_ref[r, n] = res_ref[r, n] - dot3(psh[k, r, :], psl[k, r, :], qh, ql)

    def qc(i, cx, ax, bx):
        return rc(q.at[cx, ax, bx], q.at[cx, ax, bx], qcs.at[i], qcr.at[i], dev_c)

    mine = ((a, b), (a, 1 - b), (1 - a, b), (1 - a, 1 - b))
    other = ((ap, bp), (ap, 1 - bp), (1 - ap, bp), (1 - ap, 1 - bp))

    q_step(0)
    hmix(0)
    for t in range(1, nz):
        q_step(t)
        if t < min(4, nz - 1):
            hmix(t)
    q2 = rc(q.at[core, a, b], q.at[core, a, b], q2s, q2r, dev_2)
    q2.start()
    q1 = [rc(q.at[core, a, b], q.at[core, a, b], q1s.at[0], q1r.at[0], dev_1),
          rc(q.at[core, a, 1 - b], q.at[core, a, 1 - b], q1s.at[1], q1r.at[1], dev_1)]
    q1[0].start()
    qc(0, core, *mine[0]).start()
    for i in range(min(4, nz - 1), 4):
        hmix(i)
    rc(q.at[core, a, 1 - b], q.at[core, a, 1 - b], q2s, q2r, dev_2).wait_recv()
    q1[1].start()
    qc(1, core, *mine[1]).start()
    finish(core, a)
    qc(0, pc, *other[0]).wait_recv()
    qc(1, pc, *other[1]).wait_recv()
    finish(pc, ap)
    rc(q.at[core, 1 - a, b], q.at[core, 1 - a, b], q1s.at[0], q1r.at[0], dev_1).wait_recv()
    qc(2, core, *mine[2]).start()
    rc(q.at[core, 1 - a, 1 - b], q.at[core, 1 - a, 1 - b], q1s.at[1], q1r.at[1], dev_1).wait_recv()
    qc(3, core, *mine[3]).start()
    finish(core, 1 - a)
    qc(2, pc, *other[2]).wait_recv()
    qc(3, pc, *other[3]).wait_recv()
    finish(pc, 1 - ap)

    for k in range(1, n_gcol):
        src = lax.rem(gc + n_gcol - k, n_gcol)
        r_src = pl.multiple_of((src % 2) * half + (src // 2) * each, each)
        rc(pin.at[src], proj_ref.at[pl.ds(r_src, each)], ps.at[k], pr.at[k],
           {"grow": g, "gcol": src}).wait_recv()
        sends[k - 1].wait_send()
    own_p.wait()
    for c in mc + s0 + s1 + [s2, q2] + q1:
        c.wait_send()
    for i in range(4):
        qc(i, core, *mine[i]).wait_send()
    m_drain()
    q_drain()
    for t in range(nz - 1):
        @pl.when(nz - 1 - t > z)
        def _():
            zr(t).wait_send()

        @pl.when(t < z)
        def _():
            zl(t).wait_send()


def body_kernel(psi, vpsi, kinetic, mixing):
    n_grow = lax.axis_size("grow")
    n_gcol = lax.axis_size("gcol")
    rows, nb = psi.shape
    nz = n_gcol // 2
    each = nb // (n_grow * n_gcol)
    br, bc = nb // n_grow, nb // n_gcol
    scale = 1.0 / (rows * n_grow * n_gcol)
    D = pltpu.SemaphoreType.DMA
    nch = 4
    grp = nb // 4
    V = pltpu.VMEM
    return pl.pallas_call(
        functools.partial(kernel, nz, scale),
        out_shape=(jax.ShapeDtypeStruct((rows, nb), F32), jax.ShapeDtypeStruct((br, bc), F32)),
        in_specs=[pl.BlockSpec(memory_space=pl.ANY), pl.BlockSpec(memory_space=pl.ANY),
                  pl.BlockSpec(memory_space=pltpu.VMEM), pl.BlockSpec(memory_space=pltpu.VMEM)],
        out_specs=(pl.BlockSpec(memory_space=pltpu.VMEM), pl.BlockSpec(memory_space=pltpu.VMEM)),
        scratch_shapes=[
            V((rows, nb), F32), V((rows, nb), F32),
            V((4, rows, grp), BF16), V((4, rows, grp), BF16),
            V((4, grp, rows), BF16), V((4, grp, rows), BF16),
            V((rows, nb), BF16), V((rows, nb), BF16),
            V((nb, nb), BF16), V((nb, nb), BF16),
            V((2, 2, 2, nz, each, nb), F32), V((2, 2, nz, each, nb), F32),
            V((2, nz, each, nb), F32), V((nz, each, nb), F32),
            V((nz, each, nb), F32), V((nz, each, nb), F32),
            V((n_gcol, n_grow, br, bc), F32),
            V((2, 2, 2, nz, each, nb), F32),
            V((each, nb), F32), V((n_gcol, each, bc), F32),
            D((2, nch)), D, D, D((2,)), D((2,)), D((2, nz)), D((nz,)), D((nz,)), D((nz,)), D,
            D((2,)), D((2,)), D((2,)), D((2,)), D, D, D((2, nz)), D((nz,)), D((nz,)),
            D((n_gcol,)), D((n_gcol,)), D,
            D((2, nz)), D((nz,)), D, D, D((2,)), D((2,)), D((4,)), D((4,)),
        ],
        compiler_params=pltpu.CompilerParams(
            collective_id=0, has_side_effects=True, vmem_limit_bytes=67043328),
    )(psi, vpsi, kinetic.reshape(1, rows), mixing)


def body_plain(psi, vpsi, kinetic, mixing):
    n_grow = lax.axis_size("grow")
    n_gcol = lax.axis_size("gcol")
    bands = psi.shape[1]
    scale = 1.0 / (psi.shape[0] * n_grow * n_gcol)
    dot = functools.partial(
        lax.dot_general, precision=lax.Precision.HIGHEST, preferred_element_type=F32)
    hpsi = kinetic[:, None] * psi + vpsi
    full = lax.psum(dot(psi, hpsi, (((0,), (0,)), ((), ()))) * scale, ("grow", "gcol"))
    panel = lax.all_gather(mixing, "gcol", axis=1, tiled=True)
    mix = lax.all_gather(panel, "grow", axis=0, tiled=True)
    br, bc = bands // n_grow, bands // n_gcol
    projected = lax.dynamic_slice(
        full, (lax.axis_index("grow") * br, lax.axis_index("gcol") * bc), (br, bc))
    last = (((1,), (0,)), ((), ()))
    residual = dot(hpsi - dot(psi, full, last), mix, last)
    return residual, projected


def body(psi, vpsi, kinetic, mixing):
    n_grow = lax.axis_size("grow")
    n_gcol = lax.axis_size("gcol")
    rows, nb = psi.shape
    fits = (n_grow == 2 * 2 and n_gcol % 2 == 0 and nb % (8 * n_grow * n_gcol) == 0
            and (nb // n_gcol) % 128 == 0 and (nb // n_grow) % 256 == 0 and rows % 512 == 0)
    return (body_kernel if fits else body_plain)(psi, vpsi, kinetic, mixing)


def solution(mesh):
    return jax.shard_map(
        body,
        mesh=mesh,
        in_specs=(
            P(("grow", "gcol"), None),
            P(("grow", "gcol"), None),
            P(("grow", "gcol")),
            P("grow", "gcol"),
        ),
        out_specs=(P(("grow", "gcol"), None), P("grow", "gcol")),
        check_vma=False,
    )
```

```python
import functools

import jax
import jax.numpy as jnp
from jax import lax
from jax.experimental import pallas as pl
from jax.experimental.pallas import tpu as pltpu
from jax.sharding import PartitionSpec as P

F32 = jnp.float32
BF16 = jnp.bfloat16
TN = 256


def split(x):
    hi = x.astype(BF16)
    return hi, (x - hi.astype(F32)).astype(BF16)


def dot3(ah, al, bh, bl):
    dot = functools.partial(jnp.dot, preferred_element_type=F32)
    return dot(ah, bh) + (dot(ah, bl) + dot(al, bh))


def kernel(nz, scale, psi_hbm, vpsi_hbm, kin_ref, mix_ref, res_ref, proj_ref,
           psi_v, vpsi_v, psh, psl, pth, ptl, hh, hl, mh, ml, part, r0, r1, r2,
           rzr, rzl, ma, mb, q, pown, pin,
           ld, mloc, azs, azr, a1s, a1r, a2s, a2r, b1s, b1r, b2s, b2r, bzs, bzr,
           mcs, mcr,
           s0s, s0r, s1s, s1r, s2s, s2r, zs, zrr, zrl, ps, pr, ploc,
           qzs, qzr, q2s, q2r, q1s, q1r, qcs, qcr):
    rows, nb = psi_v.shape
    n_grow = mb.shape[2]
    n_gcol = 2 * nz
    each = part.shape[4]
    bc = nb // n_gcol
    br = nb // n_grow
    half = br // 2
    grp = 2 * half
    g = lax.axis_index("grow")
    gc = lax.axis_index("gcol")
    z = gc // 2
    core = gc % 2
    pc = 1 - core
    w1 = 1 + core
    w2 = 2 - core
    a = (g // w1) % 2
    b = (g // w2) % 2
    ap, bp = b, a
    g1 = g + w1 * (1 - 2 * a)
    g2 = g + w2 * (1 - 2 * b)
    dev_c = {"grow": g, "gcol": z * 2 + pc}
    dev_1 = {"grow": g1, "gcol": gc}
    dev_2 = {"grow": g2, "gcol": gc}
    dev_r = {"grow": g, "gcol": lax.rem(gc + 2, n_gcol)}
    dev_l = {"grow": g, "gcol": lax.rem(gc + n_gcol - 2, n_gcol)}

    def rc(src, dst, ss, rs, dev):
        return pltpu.make_async_remote_copy(
            src_ref=src, dst_ref=dst, send_sem=ss, recv_sem=rs,
            device_id=dev, device_id_type=pl.DeviceIdType.MESH)

    def line(at, ss, rs):
        def right(t):
            return rc(at(z - t), at(z - t), ss.at[0, t], rs.at[z - t], dev_r)

        def left(t):
            return rc(at(z + t), at(z + t), ss.at[1, t], rs.at[z + t], dev_l)

        def step(t):
            @pl.when(z - t >= 0)
            def _():
                if t > 0:
                    rc(at(z - t), at(z - t), ss.at[0, 0], rs.at[z - t], dev_r).wait_recv()

                @pl.when(z < nz - 1)
                def _():
                    if t < nz - 1:
                        right(t).start()

            @pl.when(z + t < nz)
            def _():
                if t > 0:
                    rc(at(z + t), at(z + t), ss.at[1, 0], rs.at[z + t], dev_l).wait_recv()

                @pl.when(z > 0)
                def _():
                    if t < nz - 1:
                        left(t).start()

        def drain():
            for t in range(nz - 1):
                @pl.when((z - t >= 0) & (z < nz - 1))
                def _():
                    right(t).wait_send()

                @pl.when((z + t < nz) & (z > 0))
                def _():
                    left(t).wait_send()

        return step, drain

    nch = ld.shape[1]
    ch = rows // nch

    def loads(i):
        s = pl.ds(i * ch, ch)
        return (pltpu.make_async_copy(psi_hbm.at[s], psi_v.at[s], ld.at[0, i]),
                pltpu.make_async_copy(vpsi_hbm.at[s], vpsi_v.at[s], ld.at[1, i]))

    for i in range(nch):
        for c in loads(i):
            c.start()
    hr = br // 2
    own_m = (pltpu.make_async_copy(mix_ref.at[:hr], ma.at[core, g, z], mloc.at[0]),
             pltpu.make_async_copy(mix_ref.at[hr:], mb.at[core, z, g], mloc.at[1]))
    for c in own_m:
        c.start()

    barrier = pltpu.get_barrier_semaphore()
    for k in range(1, n_gcol):
        pl.semaphore_signal(barrier, inc=1, device_id={"grow": g, "gcol": lax.rem(gc + k, n_gcol)},
                            device_id_type=pl.DeviceIdType.MESH)
    for dev in (dev_1, dev_2):
        pl.semaphore_signal(barrier, inc=1, device_id=dev, device_id_type=pl.DeviceIdType.MESH)
    pl.semaphore_wait(barrier, n_gcol - 1 + 2)

    for c in own_m:
        c.wait()
    a_step, a_drain = line(lambda i: ma.at[core, g, i], azs, azr)
    b_step, b_drain = line(lambda i: mb.at[core, i], bzs, bzr)
    b_1 = rc(mb.at[core, z, g], mb.at[core, z, g], b1s, b1r, dev_1)
    b_1.start()
    a_step(0)

    kt = jnp.transpose(jnp.broadcast_to(kin_ref[...], (128, rows)))
    for i in range(nch):
        for c in loads(i):
            c.wait()
        r = slice(i * ch, (i + 1) * ch)
        for cc in range(2):
            for ba in range(2):
                for bb in range(2):
                    gg = (ba + 2 * bb) if cc == 0 else (2 * ba + bb)
                    for s in range(0, half, 128):
                        col = gg * br + cc * half + s
                        x = psi_v[r, col:col + 128]
                        h = kt[r, :] * x + vpsi_v[r, col:col + 128]
                        hhi, hlo = split(h)
                        hh[r, col:col + 128] = hhi
                        hl[r, col:col + 128] = hlo
                        xhi, xlo = split(x)
                        o = bb * half + s
                        k = cc * 2 + ba
                        psh[k, r, o:o + 128] = xhi
                        psl[k, r, o:o + 128] = xlo
                        pth[k, o:o + 128, r] = jnp.transpose(xhi)
                        ptl[k, o:o + 128, r] = jnp.transpose(xlo)

    b_1.wait()
    b_2 = [rc(mb.at[core, z, gx], mb.at[core, z, gx], b2s.at[k], b2r.at[k], dev_2)
           for k, gx in enumerate((g, g1))]
    for c in b_2:
        c.start()
    a_step(1)

    def mm1(cx, ax):
        k = cx * 2 + ax

        @pl.loop(0, nb // TN)
        def _(j):
            n = pl.ds(pl.multiple_of(j * TN, TN), TN)
            out = dot3(pth[k], ptl[k], hh[:, n], hl[:, n])
            part[cx, ax, :, :, :, n] = out.reshape(2, nz, each, TN)

    def s0_send(i, ax):
        c = rc(part.at[pc, ax], r0.at[i], s0s.at[i], s0r.at[i], dev_c)
        c.start()
        return c

    def m_core(i, ref):
        c = rc(ref, ref, mcs.at[i], mcr.at[i], dev_c)
        c.start()
        return c

    mm1(pc, 1 - ap)
    s0 = [s0_send(0, 1 - ap)]
    for c in b_2:
        c.wait()
    b_step(0)
    for t in range(2, nz - 1):
        a_step(t)
    mm1(core, 1 - a)
    s0[0].wait_recv()
    s1 = []
    for i, bx in enumerate((1 - b, b)):
        part[core, 1 - a, bx] = part[core, 1 - a, bx] + r0[0, bx]
        c = rc(part.at[core, 1 - a, bx], r1.at[i], s1s.at[i], s1r.at[i], dev_1)
        c.start()
        s1.append(c)
    mm1(pc, ap)
    s0.append(s0_send(1, ap))
    a_step(nz - 1)
    a_1 = rc(ma.at[core, g], ma.at[core, g], a1s, a1r, dev_1)
    a_1.start()
    mm1(core, a)
    s0[1].wait_recv()
    for bx in range(2):
        part[core, a, bx] = part[core, a, bx] + r0[1, bx]
    s1[0].wait_recv()
    part[core, a, 1 - b] = part[core, a, 1 - b] + r1[0]
    s2 = rc(part.at[core, a, 1 - b], r2, s2s, s2r, dev_2)
    s2.start()
    b_step(1)
    s1[1].wait_recv()
    part[core, a, b] = part[core, a, b] + r1[1]
    a_1.wait_recv()
    a_2 = [rc(ma.at[core, gx], ma.at[core, gx], a2s.at[k], a2r.at[k], dev_2)
           for k, gx in enumerate((g, g1))]
    for c in a_2:
        c.start()
    mc = [m_core(0, ma.at[core, g]), m_core(1, ma.at[core, g1])]
    for t in range(2, nz - 1):
        b_step(t)
    s2.wait_recv()
    part[core, a, b] = part[core, a, b] + r2[...]

    def zr(t):
        d = nz - 1 - t
        return rc(part.at[core, a, b, d], rzr.at[d], zs.at[0, t], zrr.at[d], dev_r)

    def zl(t):
        return rc(part.at[core, a, b, t], rzl.at[t], zs.at[1, t], zrl.at[t], dev_l)

    for t in range(nz):
        d = nz - 1 - t

        @pl.when((z > 0) & (d >= z))
        def _():
            rc(part.at[core, a, b, d], rzr.at[d], zs.at[0, 0], zrr.at[d], dev_r).wait_recv()
            part[core, a, b, d] = part[core, a, b, d] + rzr[d]

        if t < nz - 1:
            @pl.when(d > z)
            def _():
                zr(t).start()

        @pl.when((z < nz - 1) & (t <= z))
        def _():
            rc(part.at[core, a, b, t], rzl.at[t], zs.at[1, 0], zrl.at[t], dev_l).wait_recv()
            part[core, a, b, t] = part[core, a, b, t] + rzl[t]

        if t < nz - 1:
            @pl.when(t < z)
            def _():
                zl(t).start()

    own = part[core, a, b, z] * scale
    pown[...] = own
    for k in range(n_gcol):
        pin_k = own[:, k * bc:(k + 1) * bc]
        pin[k] = pin_k
    sends = []
    row0 = pl.multiple_of(core * half + z * each, each)
    for k in range(1, n_gcol):
        to = lax.rem(gc + k, n_gcol)
        c = rc(pin.at[to], proj_ref.at[pl.ds(row0, each)], ps.at[k], pr.at[k],
               {"grow": g, "gcol": to})
        c.start()
        sends.append(c)
    own_p = pltpu.make_async_copy(pin.at[gc], proj_ref.at[pl.ds(row0, each)], ploc)
    own_p.start()

    b_step(nz - 1)
    for i in range(nz):
        mc.append(m_core(n_grow + i, mb.at[core, i]))
    for k, (c, gx) in enumerate(zip(a_2, (g, g1))):
        c.wait_recv()
        far = gx + w2 * (1 - 2 * b)
        mc.append(m_core(2 + k, ma.at[core, far]))
    for i in range(n_grow):
        rc(ma.at[pc, i], ma.at[pc, i], mcs.at[i], mcr.at[i], dev_c).wait_recv()
    for i in range(nz):
        rc(mb.at[pc, i], mb.at[pc, i], mcs.at[n_grow + i], mcr.at[n_grow + i], dev_c).wait_recv()

    for cx in range(2):
        @pl.loop(0, nz)
        def _(k):
            n = pl.ds(pl.multiple_of((2 * k + cx) * bc, bc), bc)
            for gx in range(n_grow):
                for src, r in ((ma.at[cx, gx, k], gx * br), (mb.at[cx, k, gx], gx * br + hr)):
                    hi, lo = split(src[...])
                    mh[r:r + hr, n] = hi
                    ml[r:r + hr, n] = lo

    ph, plo = split(pown[...])

    @pl.loop(0, nb // TN)
    def _(j):
        n = pl.ds(pl.multiple_of(j * TN, TN), TN)
        q[core, a, b, z, :, n] = dot3(ph, plo, mh[:, n], ml[:, n])

    q_step, q_drain = line(lambda i: q.at[core, a, b, i], qzs, qzr)

    def hmix(i):
        @pl.loop(0, nb // TN)
        def _(j):
            n = pl.ds(pl.multiple_of(j * TN, TN), TN)
            r = slice(i * (rows // 4), (i + 1) * (rows // 4))
            res_ref[r, n] = dot3(hh[r, :], hl[r, :], mh[:, n], ml[:, n])

    def finish(cx, ax):
        k = cx * 2 + ax

        @pl.loop(0, nb // TN)
        def _(j):
            n = pl.ds(pl.multiple_of(j * TN, TN), TN)
            qh, ql = split(q[cx, ax, :, :, :, n].reshape(grp, TN))
            for i in range(4):
                r = slice(i * (rows // 4), (i + 1) * (rows // 4))
                res_ref[r, n] = res_ref[r, n] - dot3(psh[k, r, :], psl[k, r, :], qh, ql)

    def qc(i, cx, ax, bx):
        return rc(q.at[cx, ax, bx], q.at[cx, ax, bx], qcs.at[i], qcr.at[i], dev_c)

    mine = ((a, b), (a, 1 - b), (1 - a, b), (1 - a, 1 - b))
    other = ((ap, bp), (ap, 1 - bp), (1 - ap, bp), (1 - ap, 1 - bp))

    q_step(0)
    hmix(0)
    for t in range(1, nz):
        q_step(t)
        if t < min(4, nz - 1):
            hmix(t)
    q2 = rc(q.at[core, a, b], q.at[core, a, b], q2s, q2r, dev_2)
    q2.start()
    q1 = [rc(q.at[core, a, b], q.at[core, a, b], q1s.at[0], q1r.at[0], dev_1),
          rc(q.at[core, a, 1 - b], q.at[core, a, 1 - b], q1s.at[1], q1r.at[1], dev_1)]
    q1[0].start()
    qc(0, core, *mine[0]).start()
    for i in range(min(4, nz - 1), 4):
        hmix(i)
    rc(q.at[core, a, 1 - b], q.at[core, a, 1 - b], q2s, q2r, dev_2).wait_recv()
    q1[1].start()
    qc(1, core, *mine[1]).start()
    finish(core, a)
    qc(0, pc, *other[0]).wait_recv()
    qc(1, pc, *other[1]).wait_recv()
    finish(pc, ap)
    rc(q.at[core, 1 - a, b], q.at[core, 1 - a, b], q1s.at[0], q1r.at[0], dev_1).wait_recv()
    qc(2, core, *mine[2]).start()
    rc(q.at[core, 1 - a, 1 - b], q.at[core, 1 - a, 1 - b], q1s.at[1], q1r.at[1], dev_1).wait_recv()
    qc(3, core, *mine[3]).start()
    finish(core, 1 - a)
    qc(2, pc, *other[2]).wait_recv()
    qc(3, pc, *other[3]).wait_recv()
    finish(pc, 1 - ap)

    for k in range(1, n_gcol):
        src = lax.rem(gc + n_gcol - k, n_gcol)
        r_src = pl.multiple_of((src % 2) * half + (src // 2) * each, each)
        rc(pin.at[src], proj_ref.at[pl.ds(r_src, each)], ps.at[k], pr.at[k],
           {"grow": g, "gcol": src}).wait_recv()
        sends[k - 1].wait_send()
    own_p.wait()
    for c in mc + s0 + s1 + [s2, q2, a_1] + a_2 + q1:
        c.wait_send()
    for i in range(4):
        qc(i, core, *mine[i]).wait_send()
    a_drain()
    b_drain()
    q_drain()
    for t in range(nz - 1):
        @pl.when(nz - 1 - t > z)
        def _():
            zr(t).wait_send()

        @pl.when(t < z)
        def _():
            zl(t).wait_send()


def body_kernel(psi, vpsi, kinetic, mixing):
    n_grow = lax.axis_size("grow")
    n_gcol = lax.axis_size("gcol")
    rows, nb = psi.shape
    nz = n_gcol // 2
    each = nb // (n_grow * n_gcol)
    br, bc = nb // n_grow, nb // n_gcol
    scale = 1.0 / (rows * n_grow * n_gcol)
    D = pltpu.SemaphoreType.DMA
    nch = 4
    grp = nb // 4
    V = pltpu.VMEM
    return pl.pallas_call(
        functools.partial(kernel, nz, scale),
        out_shape=(V((rows, nb), F32), V((br, bc), F32)),
        in_specs=[pl.BlockSpec(memory_space=pl.ANY), pl.BlockSpec(memory_space=pl.ANY),
                  pl.BlockSpec(memory_space=pltpu.VMEM), pl.BlockSpec(memory_space=pltpu.VMEM)],
        out_specs=(pl.BlockSpec(memory_space=pltpu.VMEM), pl.BlockSpec(memory_space=pltpu.VMEM)),
        scratch_shapes=[
            V((rows, nb), F32), V((rows, nb), F32),
            V((4, rows, grp), BF16), V((4, rows, grp), BF16),
            V((4, grp, rows), BF16), V((4, grp, rows), BF16),
            V((rows, nb), BF16), V((rows, nb), BF16),
            V((nb, nb), BF16), V((nb, nb), BF16),
            V((2, 2, 2, nz, each, nb), F32), V((2, 2, nz, each, nb), F32),
            V((2, nz, each, nb), F32), V((nz, each, nb), F32),
            V((nz, each, nb), F32), V((nz, each, nb), F32),
            V((2, n_grow, nz, br // 2, bc), F32), V((2, nz, n_grow, br // 2, bc), F32),
            V((2, 2, 2, nz, each, nb), F32),
            V((each, nb), F32), V((n_gcol, each, bc), F32),
            D((2, nch)), D((2,)), D((2, nz)), D((nz,)), D, D, D((2,)), D((2,)),
            D, D, D((2,)), D((2,)), D((2, nz)), D((nz,)),
            D((n_grow + nz,)), D((n_grow + nz,)),
            D((2,)), D((2,)), D((2,)), D((2,)), D, D, D((2, nz)), D((nz,)), D((nz,)),
            D((n_gcol,)), D((n_gcol,)), D,
            D((2, nz)), D((nz,)), D, D, D((2,)), D((2,)), D((4,)), D((4,)),
        ],
        compiler_params=pltpu.CompilerParams(
            collective_id=0, has_side_effects=True, vmem_limit_bytes=52 * 2**20),
    )(psi, vpsi, kinetic.reshape(1, rows), mixing)


def body_plain(psi, vpsi, kinetic, mixing):
    n_grow = lax.axis_size("grow")
    n_gcol = lax.axis_size("gcol")
    bands = psi.shape[1]
    scale = 1.0 / (psi.shape[0] * n_grow * n_gcol)
    dot = functools.partial(
        lax.dot_general, precision=lax.Precision.HIGHEST, preferred_element_type=F32)
    hpsi = kinetic[:, None] * psi + vpsi
    full = lax.psum(dot(psi, hpsi, (((0,), (0,)), ((), ()))) * scale, ("grow", "gcol"))
    panel = lax.all_gather(mixing, "gcol", axis=1, tiled=True)
    mix = lax.all_gather(panel, "grow", axis=0, tiled=True)
    br, bc = bands // n_grow, bands // n_gcol
    projected = lax.dynamic_slice(
        full, (lax.axis_index("grow") * br, lax.axis_index("gcol") * bc), (br, bc))
    last = (((1,), (0,)), ((), ()))
    residual = dot(hpsi - dot(psi, full, last), mix, last)
    return residual, projected


def body(psi, vpsi, kinetic, mixing):
    n_grow = lax.axis_size("grow")
    n_gcol = lax.axis_size("gcol")
    rows, nb = psi.shape
    fits = (n_grow == 2 * 2 and n_gcol % 2 == 0 and nb % (8 * n_grow * n_gcol) == 0
            and (nb // n_gcol) % 128 == 0 and (nb // n_grow) % 256 == 0 and rows % 512 == 0)
    return (body_kernel if fits else body_plain)(psi, vpsi, kinetic, mixing)


def solution(mesh):
    return jax.shard_map(
        body,
        mesh=mesh,
        in_specs=(
            P(("grow", "gcol"), None),
            P(("grow", "gcol"), None),
            P(("grow", "gcol")),
            P("grow", "gcol"),
        ),
        out_specs=(P(("grow", "gcol"), None), P("grow", "gcol")),
        check_vma=False,
    )
```

```python
import functools

import jax
import jax.numpy as jnp
from jax import lax
from jax.experimental import pallas as pl
from jax.experimental.pallas import tpu as pltpu
from jax.sharding import PartitionSpec as P

F32 = jnp.float32
BF16 = jnp.bfloat16
TN = 256


def split(x):
    hi = x.astype(BF16)
    return hi, (x - hi.astype(F32)).astype(BF16)


def dot3(ah, al, bh, bl):
    dot = functools.partial(jnp.dot, preferred_element_type=F32)
    return dot(ah, bh) + (dot(ah, bl) + dot(al, bh))


def kernel(nz, scale, psi_hbm, vpsi_hbm, kin_ref, mix_ref, res_ref, proj_ref,
           psi_v, vpsi_v, psh, psl, pth, ptl, hh, hl, mh, ml, part, r0, r1, r2,
           rzr, rzl, ma, mb, q, pown, pin,
           ld, mloc, azs, azr, a1s, a1r, a2s, a2r, b1s, b1r, b2s, b2r, bzs, bzr,
           mcs, mcr,
           s0s, s0r, s1s, s1r, s2s, s2r, zs, zrr, zrl, ps, pr, ploc,
           qzs, qzr, q2s, q2r, q1s, q1r, qcs, qcr):
    rows, nb = psi_v.shape
    n_grow = mb.shape[2]
    n_gcol = 2 * nz
    each = part.shape[4]
    bc = nb // n_gcol
    br = nb // n_grow
    half = br // 2
    grp = 2 * half
    g = lax.axis_index("grow")
    gc = lax.axis_index("gcol")
    z = gc // 2
    core = gc % 2
    pc = 1 - core
    w1 = 1 + core
    w2 = 2 - core
    a = (g // w1) % 2
    b = (g // w2) % 2
    ap, bp = b, a
    g1 = g + w1 * (1 - 2 * a)
    g2 = g + w2 * (1 - 2 * b)
    dev_c = {"grow": g, "gcol": z * 2 + pc}
    dev_1 = {"grow": g1, "gcol": gc}
    dev_2 = {"grow": g2, "gcol": gc}
    dev_r = {"grow": g, "gcol": lax.rem(gc + 2, n_gcol)}
    dev_l = {"grow": g, "gcol": lax.rem(gc + n_gcol - 2, n_gcol)}

    def rc(src, dst, ss, rs, dev):
        return pltpu.make_async_remote_copy(
            src_ref=src, dst_ref=dst, send_sem=ss, recv_sem=rs,
            device_id=dev, device_id_type=pl.DeviceIdType.MESH)

    def line(at, ss, rs):
        def right(t):
            return rc(at(z - t), at(z - t), ss.at[0, t], rs.at[z - t], dev_r)

        def left(t):
            return rc(at(z + t), at(z + t), ss.at[1, t], rs.at[z + t], dev_l)

        def step(t):
            @pl.when(z - t >= 0)
            def _():
                if t > 0:
                    rc(at(z - t), at(z - t), ss.at[0, 0], rs.at[z - t], dev_r).wait_recv()

                @pl.when(z < nz - 1)
                def _():
                    if t < nz - 1:
                        right(t).start()

            @pl.when(z + t < nz)
            def _():
                if t > 0:
                    rc(at(z + t), at(z + t), ss.at[1, 0], rs.at[z + t], dev_l).wait_recv()

                @pl.when(z > 0)
                def _():
                    if t < nz - 1:
                        left(t).start()

        def drain():
            for t in range(nz - 1):
                @pl.when((z - t >= 0) & (z < nz - 1))
                def _():
                    right(t).wait_send()

                @pl.when((z + t < nz) & (z > 0))
                def _():
                    left(t).wait_send()

        return step, drain

    nch = ld.shape[1]
    ch = rows // nch

    def loads(i):
        s = pl.ds(i * ch, ch)
        return (pltpu.make_async_copy(psi_hbm.at[s], psi_v.at[s], ld.at[0, i]),
                pltpu.make_async_copy(vpsi_hbm.at[s], vpsi_v.at[s], ld.at[1, i]))

    for i in range(nch):
        for c in loads(i):
            c.start()
    hr = br // 2
    own_m = (pltpu.make_async_copy(mix_ref.at[:hr], ma.at[core, g, z], mloc.at[0]),
             pltpu.make_async_copy(mix_ref.at[hr:], mb.at[core, z, g], mloc.at[1]))
    for c in own_m:
        c.start()

    barrier = pltpu.get_barrier_semaphore()
    for k in range(1, n_gcol):
        pl.semaphore_signal(barrier, inc=1, device_id={"grow": g, "gcol": lax.rem(gc + k, n_gcol)},
                            device_id_type=pl.DeviceIdType.MESH)
    for dev in (dev_1, dev_2):
        pl.semaphore_signal(barrier, inc=1, device_id=dev, device_id_type=pl.DeviceIdType.MESH)
    pl.semaphore_wait(barrier, n_gcol - 1 + 2)

    for c in own_m:
        c.wait()
    a_step, a_drain = line(lambda i: ma.at[core, g, i], azs, azr)
    b_step, b_drain = line(lambda i: mb.at[core, i], bzs, bzr)
    b_1 = rc(mb.at[core, z, g], mb.at[core, z, g], b1s, b1r, dev_1)
    b_1.start()
    a_step(0)

    kt = jnp.transpose(jnp.broadcast_to(kin_ref[...], (128, rows)))
    for i in range(nch):
        for c in loads(i):
            c.wait()
        r = slice(i * ch, (i + 1) * ch)
        for cc in range(2):
            for ba in range(2):
                for bb in range(2):
                    gg = (ba + 2 * bb) if cc == 0 else (2 * ba + bb)
                    for s in range(0, half, 128):
                        col = gg * br + cc * half + s
                        x = psi_v[r, col:col + 128]
                        h = kt[r, :] * x + vpsi_v[r, col:col + 128]
                        hhi, hlo = split(h)
                        hh[r, col:col + 128] = hhi
                        hl[r, col:col + 128] = hlo
                        xhi, xlo = split(x)
                        o = bb * half + s
                        k = cc * 2 + ba
                        psh[k, r, o:o + 128] = xhi
                        psl[k, r, o:o + 128] = xlo
                        pth[k, o:o + 128, r] = jnp.transpose(xhi)
                        ptl[k, o:o + 128, r] = jnp.transpose(xlo)

    b_1.wait()
    b_2 = [rc(mb.at[core, z, gx], mb.at[core, z, gx], b2s.at[k], b2r.at[k], dev_2)
           for k, gx in enumerate((g, g1))]
    for c in b_2:
        c.start()
    a_step(1)

    def mm1(cx, ax):
        k = cx * 2 + ax

        @pl.loop(0, nb // TN)
        def _(j):
            n = pl.ds(pl.multiple_of(j * TN, TN), TN)
            out = dot3(pth[k], ptl[k], hh[:, n], hl[:, n])
            part[cx, ax, :, :, :, n] = out.reshape(2, nz, each, TN)

    def s0_send(i, ax):
        c = rc(part.at[pc, ax], r0.at[i], s0s.at[i], s0r.at[i], dev_c)
        c.start()
        return c

    def m_core(i, ref):
        c = rc(ref, ref, mcs.at[i], mcr.at[i], dev_c)
        c.start()
        return c

    mm1(pc, 1 - ap)
    s0 = [s0_send(0, 1 - ap)]
    for c in b_2:
        c.wait()
    b_step(0)
    for t in range(2, nz - 1):
        a_step(t)
    mm1(core, 1 - a)
    s0[0].wait_recv()
    s1 = []
    for i, bx in enumerate((1 - b, b)):
        part[core, 1 - a, bx] = part[core, 1 - a, bx] + r0[0, bx]
        c = rc(part.at[core, 1 - a, bx], r1.at[i], s1s.at[i], s1r.at[i], dev_1)
        c.start()
        s1.append(c)
    mm1(pc, ap)
    s0.append(s0_send(1, ap))
    a_step(nz - 1)
    a_1 = rc(ma.at[core, g], ma.at[core, g], a1s, a1r, dev_1)
    a_1.start()
    b_step(1)
    mm1(core, a)
    s0[1].wait_recv()
    for bx in range(2):
        part[core, a, bx] = part[core, a, bx] + r0[1, bx]
    s1[0].wait_recv()
    part[core, a, 1 - b] = part[core, a, 1 - b] + r1[0]
    s2 = rc(part.at[core, a, 1 - b], r2, s2s, s2r, dev_2)
    s2.start()
    for t in range(2, nz - 1):
        b_step(t)
    s1[1].wait_recv()
    part[core, a, b] = part[core, a, b] + r1[1]
    s2.wait_recv()
    part[core, a, b] = part[core, a, b] + r2[...]

    def zsum(buf, ss, rs, dev, d):
        return rc(part.at[core, a, b, d], buf.at[d], ss, rs.at[d], dev)

    for tick in range(2 * nz - 1):
        if tick == 1:
            a_1.wait_recv()
            a_2 = [rc(ma.at[core, gx], ma.at[core, gx], a2s.at[k], a2r.at[k], dev_2)
                   for k, gx in enumerate((g, g1))]
            for c in a_2:
                c.start()
            mc = [m_core(0, ma.at[core, g]), m_core(1, ma.at[core, g1])]
        dr = nz - 1 - (tick - z)
        dl = tick - (nz - 1 - z)

        @pl.when((dr <= nz - 1) & (dr >= z) & (z > 0))
        def _():
            zsum(rzr, zs.at[0, 0], zrr, dev_r, dr).wait_recv()
            part[core, a, b, dr] = part[core, a, b, dr] + rzr[dr]

        @pl.when((dr <= nz - 1) & (dr > z))
        def _():
            zsum(rzr, zs.at[0, dr], zrr, dev_r, dr).start()

        @pl.when((dl >= 0) & (dl <= z) & (z < nz - 1))
        def _():
            zsum(rzl, zs.at[1, 0], zrl, dev_l, dl).wait_recv()
            part[core, a, b, dl] = part[core, a, b, dl] + rzl[dl]

        @pl.when((dl >= 0) & (dl < z))
        def _():
            zsum(rzl, zs.at[1, dl], zrl, dev_l, dl).start()

    own = part[core, a, b, z] * scale
    pown[...] = own
    for k in range(n_gcol):
        pin_k = own[:, k * bc:(k + 1) * bc]
        pin[k] = pin_k
    sends = []
    row0 = pl.multiple_of(core * half + z * each, each)
    for k in range(1, n_gcol):
        to = lax.rem(gc + k, n_gcol)
        c = rc(pin.at[to], proj_ref.at[pl.ds(row0, each)], ps.at[k], pr.at[k],
               {"grow": g, "gcol": to})
        c.start()
        sends.append(c)
    own_p = pltpu.make_async_copy(pin.at[gc], proj_ref.at[pl.ds(row0, each)], ploc)
    own_p.start()

    b_step(nz - 1)
    for i in range(nz):
        mc.append(m_core(n_grow + i, mb.at[core, i]))
    for k, (c, gx) in enumerate(zip(a_2, (g, g1))):
        c.wait_recv()
        far = gx + w2 * (1 - 2 * b)
        mc.append(m_core(2 + k, ma.at[core, far]))
    for i in range(n_grow):
        rc(ma.at[pc, i], ma.at[pc, i], mcs.at[i], mcr.at[i], dev_c).wait_recv()
    for i in range(nz):
        rc(mb.at[pc, i], mb.at[pc, i], mcs.at[n_grow + i], mcr.at[n_grow + i], dev_c).wait_recv()

    for cx in range(2):
        @pl.loop(0, nz)
        def _(k):
            n = pl.ds(pl.multiple_of((2 * k + cx) * bc, bc), bc)
            for gx in range(n_grow):
                for src, r in ((ma.at[cx, gx, k], gx * br), (mb.at[cx, k, gx], gx * br + hr)):
                    hi, lo = split(src[...])
                    mh[r:r + hr, n] = hi
                    ml[r:r + hr, n] = lo

    ph, plo = split(pown[...])

    @pl.loop(0, nb // TN)
    def _(j):
        n = pl.ds(pl.multiple_of(j * TN, TN), TN)
        q[core, a, b, z, :, n] = dot3(ph, plo, mh[:, n], ml[:, n])

    q_step, q_drain = line(lambda i: q.at[core, a, b, i], qzs, qzr)

    def hmix(i):
        @pl.loop(0, nb // TN)
        def _(j):
            n = pl.ds(pl.multiple_of(j * TN, TN), TN)
            r = slice(i * (rows // 4), (i + 1) * (rows // 4))
            res_ref[r, n] = dot3(hh[r, :], hl[r, :], mh[:, n], ml[:, n])

    def finish(cx, ax):
        k = cx * 2 + ax

        @pl.loop(0, nb // TN)
        def _(j):
            n = pl.ds(pl.multiple_of(j * TN, TN), TN)
            qh, ql = split(q[cx, ax, :, :, :, n].reshape(grp, TN))
            for i in range(4):
                r = slice(i * (rows // 4), (i + 1) * (rows // 4))
                res_ref[r, n] = res_ref[r, n] - dot3(psh[k, r, :], psl[k, r, :], qh, ql)

    def qc(i, cx, ax, bx):
        return rc(q.at[cx, ax, bx], q.at[cx, ax, bx], qcs.at[i], qcr.at[i], dev_c)

    mine = ((a, b), (a, 1 - b), (1 - a, b), (1 - a, 1 - b))
    other = ((ap, bp), (ap, 1 - bp), (1 - ap, bp), (1 - ap, 1 - bp))

    q_step(0)
    hmix(0)
    for t in range(1, nz):
        q_step(t)
        if t < min(4, nz - 1):
            hmix(t)
    q2 = rc(q.at[core, a, b], q.at[core, a, b], q2s, q2r, dev_2)
    q2.start()
    q1 = [rc(q.at[core, a, b], q.at[core, a, b], q1s.at[0], q1r.at[0], dev_1),
          rc(q.at[core, a, 1 - b], q.at[core, a, 1 - b], q1s.at[1], q1r.at[1], dev_1)]
    q1[0].start()
    qc(0, core, *mine[0]).start()
    for i in range(min(4, nz - 1), 4):
        hmix(i)
    rc(q.at[core, a, 1 - b], q.at[core, a, 1 - b], q2s, q2r, dev_2).wait_recv()
    q1[1].start()
    qc(1, core, *mine[1]).start()
    finish(core, a)
    qc(0, pc, *other[0]).wait_recv()
    qc(1, pc, *other[1]).wait_recv()
    finish(pc, ap)
    rc(q.at[core, 1 - a, b], q.at[core, 1 - a, b], q1s.at[0], q1r.at[0], dev_1).wait_recv()
    qc(2, core, *mine[2]).start()
    rc(q.at[core, 1 - a, 1 - b], q.at[core, 1 - a, 1 - b], q1s.at[1], q1r.at[1], dev_1).wait_recv()
    qc(3, core, *mine[3]).start()
    finish(core, 1 - a)
    qc(2, pc, *other[2]).wait_recv()
    qc(3, pc, *other[3]).wait_recv()
    finish(pc, 1 - ap)

    for k in range(1, n_gcol):
        src = lax.rem(gc + n_gcol - k, n_gcol)
        r_src = pl.multiple_of((src % 2) * half + (src // 2) * each, each)
        rc(pin.at[src], proj_ref.at[pl.ds(r_src, each)], ps.at[k], pr.at[k],
           {"grow": g, "gcol": src}).wait_recv()
        sends[k - 1].wait_send()
    own_p.wait()
    for c in mc + s0 + s1 + [s2, q2, a_1] + a_2 + q1:
        c.wait_send()
    for i in range(4):
        qc(i, core, *mine[i]).wait_send()
    a_drain()
    b_drain()
    q_drain()
    for d in range(nz):
        @pl.when(d > z)
        def _():
            zsum(rzr, zs.at[0, d], zrr, dev_r, d).wait_send()

        @pl.when(d < z)
        def _():
            zsum(rzl, zs.at[1, d], zrl, dev_l, d).wait_send()


def body_kernel(psi, vpsi, kinetic, mixing):
    n_grow = lax.axis_size("grow")
    n_gcol = lax.axis_size("gcol")
    rows, nb = psi.shape
    nz = n_gcol // 2
    each = nb // (n_grow * n_gcol)
    br, bc = nb // n_grow, nb // n_gcol
    scale = 1.0 / (rows * n_grow * n_gcol)
    D = pltpu.SemaphoreType.DMA
    nch = 4
    grp = nb // 4
    V = pltpu.VMEM
    return pl.pallas_call(
        functools.partial(kernel, nz, scale),
        out_shape=(V((rows, nb), F32), V((br, bc), F32)),
        in_specs=[pl.BlockSpec(memory_space=pl.ANY), pl.BlockSpec(memory_space=pl.ANY),
                  pl.BlockSpec(memory_space=pltpu.VMEM), pl.BlockSpec(memory_space=pltpu.VMEM)],
        out_specs=(pl.BlockSpec(memory_space=pltpu.VMEM), pl.BlockSpec(memory_space=pltpu.VMEM)),
        scratch_shapes=[
            V((rows, nb), F32), V((rows, nb), F32),
            V((4, rows, grp), BF16), V((4, rows, grp), BF16),
            V((4, grp, rows), BF16), V((4, grp, rows), BF16),
            V((rows, nb), BF16), V((rows, nb), BF16),
            V((nb, nb), BF16), V((nb, nb), BF16),
            V((2, 2, 2, nz, each, nb), F32), V((2, 2, nz, each, nb), F32),
            V((2, nz, each, nb), F32), V((nz, each, nb), F32),
            V((nz, each, nb), F32), V((nz, each, nb), F32),
            V((2, n_grow, nz, br // 2, bc), F32), V((2, nz, n_grow, br // 2, bc), F32),
            V((2, 2, 2, nz, each, nb), F32),
            V((each, nb), F32), V((n_gcol, each, bc), F32),
            D((2, nch)), D((2,)), D((2, nz)), D((nz,)), D, D, D((2,)), D((2,)),
            D, D, D((2,)), D((2,)), D((2, nz)), D((nz,)),
            D((n_grow + nz,)), D((n_grow + nz,)),
            D((2,)), D((2,)), D((2,)), D((2,)), D, D, D((2, nz)), D((nz,)), D((nz,)),
            D((n_gcol,)), D((n_gcol,)), D,
            D((2, nz)), D((nz,)), D, D, D((2,)), D((2,)), D((4,)), D((4,)),
        ],
        compiler_params=pltpu.CompilerParams(
            collective_id=0, has_side_effects=True, vmem_limit_bytes=52 * 2**20),
    )(psi, vpsi, kinetic.reshape(1, rows), mixing)


def body_plain(psi, vpsi, kinetic, mixing):
    n_grow = lax.axis_size("grow")
    n_gcol = lax.axis_size("gcol")
    bands = psi.shape[1]
    scale = 1.0 / (psi.shape[0] * n_grow * n_gcol)
    dot = functools.partial(
        lax.dot_general, precision=lax.Precision.HIGHEST, preferred_element_type=F32)
    hpsi = kinetic[:, None] * psi + vpsi
    full = lax.psum(dot(psi, hpsi, (((0,), (0,)), ((), ()))) * scale, ("grow", "gcol"))
    panel = lax.all_gather(mixing, "gcol", axis=1, tiled=True)
    mix = lax.all_gather(panel, "grow", axis=0, tiled=True)
    br, bc = bands // n_grow, bands // n_gcol
    projected = lax.dynamic_slice(
        full, (lax.axis_index("grow") * br, lax.axis_index("gcol") * bc), (br, bc))
    last = (((1,), (0,)), ((), ()))
    residual = dot(hpsi - dot(psi, full, last), mix, last)
    return residual, projected


def body(psi, vpsi, kinetic, mixing):
    n_grow = lax.axis_size("grow")
    n_gcol = lax.axis_size("gcol")
    rows, nb = psi.shape
    fits = (n_grow == 2 * 2 and n_gcol % 2 == 0 and nb % (8 * n_grow * n_gcol) == 0
            and (nb // n_gcol) % 128 == 0 and (nb // n_grow) % 256 == 0 and rows % 512 == 0)
    return (body_kernel if fits else body_plain)(psi, vpsi, kinetic, mixing)


def solution(mesh):
    return jax.shard_map(
        body,
        mesh=mesh,
        in_specs=(
            P(("grow", "gcol"), None),
            P(("grow", "gcol"), None),
            P(("grow", "gcol")),
            P("grow", "gcol"),
        ),
        out_specs=(P(("grow", "gcol"), None), P("grow", "gcol")),
        check_vma=False,
    )
```

```python
import functools

import jax
import jax.numpy as jnp
from jax import lax
from jax.experimental import pallas as pl
from jax.experimental.pallas import tpu as pltpu
from jax.sharding import PartitionSpec as P

F32 = jnp.float32
BF16 = jnp.bfloat16
TN = 256


def split(x):
    hi = x.astype(BF16)
    return hi, (x - hi.astype(F32)).astype(BF16)


def dot3(ah, al, bh, bl):
    dot = functools.partial(jnp.dot, preferred_element_type=F32)
    return dot(ah, bh) + (dot(ah, bl) + dot(al, bh))


def kernel(nz, scale, psi_hbm, vpsi_hbm, kin_ref, mix_ref, res_ref, proj_ref,
           psi_v, vpsi_v, psh, psl, pth, ptl, hh, hl, mh, ml, part, r0, r1, r2,
           rzr, rzl, ma, mb, q, pown, pin,
           ld, mloc, azs, azr, a1s, a1r, a2s, a2r, b1s, b1r, b2s, b2r, bzs, bzr,
           mcs, mcr,
           s0s, s0r, s1s, s1r, s2s, s2r, zs, zrr, zrl, ps, pr, ploc,
           qzs, qzr, q2s, q2r, q1s, q1r, qcs, qcr,
           e1s, e1r, e2s, e2r, ezs, ezr, ecs, ecr):
    rows, nb = psi_v.shape
    n_grow = mb.shape[2]
    n_gcol = 2 * nz
    each = part.shape[4]
    bc = nb // n_gcol
    br = nb // n_grow
    half = br // 2
    grp = 2 * half
    g = lax.axis_index("grow")
    gc = lax.axis_index("gcol")
    z = gc // 2
    core = gc % 2
    pc = 1 - core
    w1 = 1 + core
    w2 = 2 - core
    a = (g // w1) % 2
    b = (g // w2) % 2
    ap, bp = b, a
    g1 = g + w1 * (1 - 2 * a)
    g2 = g + w2 * (1 - 2 * b)
    dev_c = {"grow": g, "gcol": z * 2 + pc}
    dev_1 = {"grow": g1, "gcol": gc}
    dev_2 = {"grow": g2, "gcol": gc}
    dev_r = {"grow": g, "gcol": lax.rem(gc + 2, n_gcol)}
    dev_l = {"grow": g, "gcol": lax.rem(gc + n_gcol - 2, n_gcol)}

    def rc(src, dst, ss, rs, dev):
        return pltpu.make_async_remote_copy(
            src_ref=src, dst_ref=dst, send_sem=ss, recv_sem=rs,
            device_id=dev, device_id_type=pl.DeviceIdType.MESH)

    def line(at, ss, rs):
        def right(t):
            return rc(at(z - t), at(z - t), ss.at[0, t], rs.at[z - t], dev_r)

        def left(t):
            return rc(at(z + t), at(z + t), ss.at[1, t], rs.at[z + t], dev_l)

        def step(t):
            @pl.when(z - t >= 0)
            def _():
                if t > 0:
                    rc(at(z - t), at(z - t), ss.at[0, 0], rs.at[z - t], dev_r).wait_recv()

                @pl.when(z < nz - 1)
                def _():
                    if t < nz - 1:
                        right(t).start()

            @pl.when(z + t < nz)
            def _():
                if t > 0:
                    rc(at(z + t), at(z + t), ss.at[1, 0], rs.at[z + t], dev_l).wait_recv()

                @pl.when(z > 0)
                def _():
                    if t < nz - 1:
                        left(t).start()

        def drain():
            for t in range(nz - 1):
                @pl.when((z - t >= 0) & (z < nz - 1))
                def _():
                    right(t).wait_send()

                @pl.when((z + t < nz) & (z > 0))
                def _():
                    left(t).wait_send()

        return step, drain

    nch = ld.shape[1]
    ch = rows // nch

    def loads(i):
        s = pl.ds(i * ch, ch)
        return (pltpu.make_async_copy(psi_hbm.at[s], psi_v.at[s], ld.at[0, i]),
                pltpu.make_async_copy(vpsi_hbm.at[s], vpsi_v.at[s], ld.at[1, i]))

    for i in range(nch):
        for c in loads(i):
            c.start()
    hr = br // 2
    own_m = (pltpu.make_async_copy(mix_ref.at[:hr], ma.at[core, g, z], mloc.at[0]),
             pltpu.make_async_copy(mix_ref.at[hr:], mb.at[core, z, g], mloc.at[1]))
    for c in own_m:
        c.start()

    barrier = pltpu.get_barrier_semaphore()
    for k in range(1, n_gcol):
        pl.semaphore_signal(barrier, inc=1, device_id={"grow": g, "gcol": lax.rem(gc + k, n_gcol)},
                            device_id_type=pl.DeviceIdType.MESH)
    for dev in (dev_1, dev_2):
        pl.semaphore_signal(barrier, inc=1, device_id=dev, device_id_type=pl.DeviceIdType.MESH)
    pl.semaphore_wait(barrier, n_gcol - 1 + 2)

    for c in own_m:
        c.wait()
    a_step, a_drain = line(lambda i: ma.at[core, g, i], azs, azr)
    b_step, b_drain = line(lambda i: mb.at[core, i], bzs, bzr)
    b_1 = rc(mb.at[core, z, g], mb.at[core, z, g], b1s, b1r, dev_1)
    b_1.start()
    a_step(0)

    kt = jnp.transpose(jnp.broadcast_to(kin_ref[...], (128, rows)))
    for i in range(nch):
        for c in loads(i):
            c.wait()
        r = slice(i * ch, (i + 1) * ch)
        for cc in range(2):
            for ba in range(2):
                for bb in range(2):
                    gg = (ba + 2 * bb) if cc == 0 else (2 * ba + bb)
                    for s in range(0, half, 128):
                        col = gg * br + cc * half + s
                        x = psi_v[r, col:col + 128]
                        h = kt[r, :] * x + vpsi_v[r, col:col + 128]
                        hhi, hlo = split(h)
                        hh[r, col:col + 128] = hhi
                        hl[r, col:col + 128] = hlo
                        xhi, xlo = split(x)
                        o = bb * half + s
                        k = cc * 2 + ba
                        psh[k, r, o:o + 128] = xhi
                        psl[k, r, o:o + 128] = xlo
                        pth[k, o:o + 128, r] = jnp.transpose(xhi)
                        ptl[k, o:o + 128, r] = jnp.transpose(xlo)

    b_1.wait()
    b_2 = [rc(mb.at[core, z, gx], mb.at[core, z, gx], b2s.at[k], b2r.at[k], dev_2)
           for k, gx in enumerate((g, g1))]
    for c in b_2:
        c.start()
    a_step(1)

    def mm1(cx, ax):
        k = cx * 2 + ax

        @pl.loop(0, nb // TN)
        def _(j):
            n = pl.ds(pl.multiple_of(j * TN, TN), TN)
            out = dot3(pth[k], ptl[k], hh[:, n], hl[:, n])
            part[cx, ax, :, :, :, n] = out.reshape(2, nz, each, TN)

    def s0_send(i, ax):
        c = rc(part.at[pc, ax], r0.at[i], s0s.at[i], s0r.at[i], dev_c)
        c.start()
        return c

    def m_core(i, ref):
        c = rc(ref, ref, mcs.at[i], mcr.at[i], dev_c)
        c.start()
        return c

    mm1(pc, 1 - ap)
    s0 = [s0_send(0, 1 - ap)]
    for c in b_2:
        c.wait()
    b_step(0)
    for t in range(2, nz - 1):
        a_step(t)
    mm1(core, 1 - a)
    s0[0].wait_recv()
    s1 = []
    for i, bx in enumerate((1 - b, b)):
        part[core, 1 - a, bx] = part[core, 1 - a, bx] + r0[0, bx]
        c = rc(part.at[core, 1 - a, bx], r1.at[i], s1s.at[i], s1r.at[i], dev_1)
        c.start()
        s1.append(c)
    mm1(pc, ap)
    s0.append(s0_send(1, ap))
    a_step(nz - 1)
    a_1 = rc(ma.at[core, g], ma.at[core, g], a1s, a1r, dev_1)
    a_1.start()
    b_step(1)
    mm1(core, a)
    s0[1].wait_recv()
    for bx in range(2):
        part[core, a, bx] = part[core, a, bx] + r0[1, bx]
    s1[0].wait_recv()
    part[core, a, 1 - b] = part[core, a, 1 - b] + r1[0]
    s2 = rc(part.at[core, a, 1 - b], r2, s2s, s2r, dev_2)
    s2.start()
    for t in range(2, nz - 1):
        b_step(t)
    s1[1].wait_recv()
    part[core, a, b] = part[core, a, b] + r1[1]
    s2.wait_recv()
    part[core, a, b] = part[core, a, b] + r2[...]

    def zsum(buf, ss, rs, dev, d):
        return rc(part.at[core, a, b, d], buf.at[d], ss, rs.at[d], dev)

    for tick in range(2 * nz - 1):
        if tick == 1:
            a_1.wait_recv()
            a_2 = [rc(ma.at[core, gx], ma.at[core, gx], a2s.at[k], a2r.at[k], dev_2)
                   for k, gx in enumerate((g, g1))]
            for c in a_2:
                c.start()
            mc = [m_core(0, ma.at[core, g]), m_core(1, ma.at[core, g1])]
        dr = nz - 1 - (tick - z)
        dl = tick - (nz - 1 - z)

        @pl.when((dr <= nz - 1) & (dr >= z) & (z > 0))
        def _():
            zsum(rzr, zs.at[0, 0], zrr, dev_r, dr).wait_recv()
            part[core, a, b, dr] = part[core, a, b, dr] + rzr[dr]

        @pl.when((dr <= nz - 1) & (dr > z))
        def _():
            zsum(rzr, zs.at[0, dr], zrr, dev_r, dr).start()

        @pl.when((dl >= 0) & (dl <= z) & (z < nz - 1))
        def _():
            zsum(rzl, zs.at[1, 0], zrl, dev_l, dl).wait_recv()
            part[core, a, b, dl] = part[core, a, b, dl] + rzl[dl]

        @pl.when((dl >= 0) & (dl < z))
        def _():
            zsum(rzl, zs.at[1, dl], zrl, dev_l, dl).start()

    own = part[core, a, b, z] * scale
    pown[...] = own
    for k in range(n_gcol):
        pin_k = own[:, k * bc:(k + 1) * bc]
        pin[k] = pin_k
    sends = []
    row0 = pl.multiple_of(core * half + z * each, each)
    for k in range(1, n_gcol):
        to = lax.rem(gc + k, n_gcol)
        c = rc(pin.at[to], proj_ref.at[pl.ds(row0, each)], ps.at[k], pr.at[k],
               {"grow": g, "gcol": to})
        c.start()
        sends.append(c)
    own_p = pltpu.make_async_copy(pin.at[gc], proj_ref.at[pl.ds(row0, each)], ploc)
    own_p.start()

    b_step(nz - 1)
    for i in range(nz):
        mc.append(m_core(n_grow + i, mb.at[core, i]))
    for k, (c, gx) in enumerate(zip(a_2, (g, g1))):
        c.wait_recv()
        far = gx + w2 * (1 - 2 * b)
        mc.append(m_core(2 + k, ma.at[core, far]))
    for i in range(n_grow):
        rc(ma.at[pc, i], ma.at[pc, i], mcs.at[i], mcr.at[i], dev_c).wait_recv()
    for i in range(nz):
        rc(mb.at[pc, i], mb.at[pc, i], mcs.at[n_grow + i], mcr.at[n_grow + i], dev_c).wait_recv()

    for cx in range(2):
        @pl.loop(0, nz)
        def _(k):
            n = pl.ds(pl.multiple_of((2 * k + cx) * bc, bc), bc)
            for gx in range(n_grow):
                for src, r in ((ma.at[cx, gx, k], gx * br), (mb.at[cx, k, gx], gx * br + hr)):
                    hi, lo = split(src[...])
                    mh[r:r + hr, n] = hi
                    ml[r:r + hr, n] = lo

    ph, plo = split(pown[...])

    @pl.loop(0, nb // TN)
    def _(j):
        n = pl.ds(pl.multiple_of(j * TN, TN), TN)
        q[core, a, b, z, :, n] = dot3(ph, plo, mh[:, n], ml[:, n])

    cut = nb - (3 * nb // 8) // 128 * 128
    A = slice(0, cut)
    B = slice(cut, nb)
    q_step, q_drain = line(lambda i: q.at[core, a, b, i, :, A], qzs, qzr)
    e_step, e_drain = line(lambda i: q.at[core, :, :, i, :, B], ezs, ezr)

    def hmix(i):
        @pl.loop(0, nb // TN)
        def _(j):
            n = pl.ds(pl.multiple_of(j * TN, TN), TN)
            r = slice(i * (rows // 4), (i + 1) * (rows // 4))
            res_ref[r, n] = dot3(hh[r, :], hl[r, :], mh[:, n], ml[:, n])

    def finish(cx, ax, n):
        k = cx * 2 + ax
        qh, ql = split(q[cx, ax, :, :, :, n].reshape(grp, n.stop - n.start))
        for i in range(4):
            r = slice(i * (rows // 4), (i + 1) * (rows // 4))
            res_ref[r, n] = res_ref[r, n] - dot3(psh[k, r, :], psl[k, r, :], qh, ql)

    def qc(i, cx, ax, bx):
        at = q.at[cx, ax, bx, :, :, A]
        return rc(at, at, qcs.at[i], qcr.at[i], dev_c)

    def ec(i, cx):
        at = q.at[cx, :, :, i, :, B]
        return rc(at, at, ecs.at[i], ecr.at[i], dev_c)

    def q_send(ax, bx, ss, rs, dev):
        at = q.at[core, ax, bx, :, :, A]
        return rc(at, at, ss, rs, dev)

    def e_send(ax, ss, rs, dev):
        at = q.at[core, ax, b, z, :, B]
        return rc(at, at, ss, rs, dev)

    mine = ((a, b), (a, 1 - b), (1 - a, b), (1 - a, 1 - b))
    other = ((ap, bp), (ap, 1 - bp), (1 - ap, bp), (1 - ap, 1 - bp))

    e1 = e_send(a, e1s, e1r, dev_1)
    e1.start()
    q_step(0)
    hmix(0)
    e1.wait_recv()
    e2 = [e_send(ax, e2s.at[i], e2r.at[i], dev_2) for i, ax in enumerate((a, 1 - a))]
    for c in e2:
        c.start()
    q_step(1)
    hmix(1)
    for t in range(2, nz - 1):
        q_step(t)
    for c in e2:
        c.wait_recv()
    e_step(0)
    hmix(2)
    q_step(nz - 1)
    q2 = q_send(a, b, q2s, q2r, dev_2)
    q2.start()
    q1 = [q_send(a, b, q1s.at[0], q1r.at[0], dev_1),
          q_send(a, 1 - b, q1s.at[1], q1r.at[1], dev_1)]
    q1[0].start()
    qc(0, core, *mine[0]).start()
    hmix(3)
    e_step(1)
    q_send(a, 1 - b, q2s, q2r, dev_2).wait_recv()
    q1[1].start()
    qc(1, core, *mine[1]).start()
    for t in range(2, nz - 1):
        e_step(t)
    finish(core, a, A)
    qc(0, pc, *other[0]).wait_recv()
    qc(1, pc, *other[1]).wait_recv()
    finish(pc, ap, A)
    e_step(nz - 1)
    ecs_own = [ec(i, core) for i in range(nz)]
    for c in ecs_own:
        c.start()
    q_send(1 - a, b, q1s.at[0], q1r.at[0], dev_1).wait_recv()
    qc(2, core, *mine[2]).start()
    finish(core, 0, B)
    q_send(1 - a, 1 - b, q1s.at[1], q1r.at[1], dev_1).wait_recv()
    qc(3, core, *mine[3]).start()
    finish(core, 1, B)
    finish(core, 1 - a, A)
    for i in range(nz):
        ec(i, pc).wait_recv()
    finish(pc, 0, B)
    finish(pc, 1, B)
    qc(2, pc, *other[2]).wait_recv()
    qc(3, pc, *other[3]).wait_recv()
    finish(pc, 1 - ap, A)

    for k in range(1, n_gcol):
        src = lax.rem(gc + n_gcol - k, n_gcol)
        r_src = pl.multiple_of((src % 2) * half + (src // 2) * each, each)
        rc(pin.at[src], proj_ref.at[pl.ds(r_src, each)], ps.at[k], pr.at[k],
           {"grow": g, "gcol": src}).wait_recv()
        sends[k - 1].wait_send()
    own_p.wait()
    for c in mc + s0 + s1 + [s2, q2, a_1, e1] + a_2 + q1 + e2 + ecs_own:
        c.wait_send()
    for i in range(4):
        qc(i, core, *mine[i]).wait_send()
    a_drain()
    b_drain()
    q_drain()
    e_drain()
    for d in range(nz):
        @pl.when(d > z)
        def _():
            zsum(rzr, zs.at[0, d], zrr, dev_r, d).wait_send()

        @pl.when(d < z)
        def _():
            zsum(rzl, zs.at[1, d], zrl, dev_l, d).wait_send()


def body_kernel(psi, vpsi, kinetic, mixing):
    n_grow = lax.axis_size("grow")
    n_gcol = lax.axis_size("gcol")
    rows, nb = psi.shape
    nz = n_gcol // 2
    each = nb // (n_grow * n_gcol)
    br, bc = nb // n_grow, nb // n_gcol
    scale = 1.0 / (rows * n_grow * n_gcol)
    D = pltpu.SemaphoreType.DMA
    nch = 4
    grp = nb // 4
    V = pltpu.VMEM
    return pl.pallas_call(
        functools.partial(kernel, nz, scale),
        out_shape=(V((rows, nb), F32), V((br, bc), F32)),
        in_specs=[pl.BlockSpec(memory_space=pl.ANY), pl.BlockSpec(memory_space=pl.ANY),
                  pl.BlockSpec(memory_space=pltpu.VMEM), pl.BlockSpec(memory_space=pltpu.VMEM)],
        out_specs=(pl.BlockSpec(memory_space=pltpu.VMEM), pl.BlockSpec(memory_space=pltpu.VMEM)),
        scratch_shapes=[
            V((rows, nb), F32), V((rows, nb), F32),
            V((4, rows, grp), BF16), V((4, rows, grp), BF16),
            V((4, grp, rows), BF16), V((4, grp, rows), BF16),
            V((rows, nb), BF16), V((rows, nb), BF16),
            V((nb, nb), BF16), V((nb, nb), BF16),
            V((2, 2, 2, nz, each, nb), F32), V((2, 2, nz, each, nb), F32),
            V((2, nz, each, nb), F32), V((nz, each, nb), F32),
            V((nz, each, nb), F32), V((nz, each, nb), F32),
            V((2, n_grow, nz, br // 2, bc), F32), V((2, nz, n_grow, br // 2, bc), F32),
            V((2, 2, 2, nz, each, nb), F32),
            V((each, nb), F32), V((n_gcol, each, bc), F32),
            D((2, nch)), D((2,)), D((2, nz)), D((nz,)), D, D, D((2,)), D((2,)),
            D, D, D((2,)), D((2,)), D((2, nz)), D((nz,)),
            D((n_grow + nz,)), D((n_grow + nz,)),
            D((2,)), D((2,)), D((2,)), D((2,)), D, D, D((2, nz)), D((nz,)), D((nz,)),
            D((n_gcol,)), D((n_gcol,)), D,
            D((2, nz)), D((nz,)), D, D, D((2,)), D((2,)), D((4,)), D((4,)),
            D, D, D((2,)), D((2,)), D((2, nz)), D((nz,)), D((nz,)), D((nz,)),
        ],
        compiler_params=pltpu.CompilerParams(
            collective_id=0, has_side_effects=True, vmem_limit_bytes=52 * 2**20),
    )(psi, vpsi, kinetic.reshape(1, rows), mixing)


def body_plain(psi, vpsi, kinetic, mixing):
    n_grow = lax.axis_size("grow")
    n_gcol = lax.axis_size("gcol")
    bands = psi.shape[1]
    scale = 1.0 / (psi.shape[0] * n_grow * n_gcol)
    dot = functools.partial(
        lax.dot_general, precision=lax.Precision.HIGHEST, preferred_element_type=F32)
    hpsi = kinetic[:, None] * psi + vpsi
    full = lax.psum(dot(psi, hpsi, (((0,), (0,)), ((), ()))) * scale, ("grow", "gcol"))
    panel = lax.all_gather(mixing, "gcol", axis=1, tiled=True)
    mix = lax.all_gather(panel, "grow", axis=0, tiled=True)
    br, bc = bands // n_grow, bands // n_gcol
    projected = lax.dynamic_slice(
        full, (lax.axis_index("grow") * br, lax.axis_index("gcol") * bc), (br, bc))
    last = (((1,), (0,)), ((), ()))
    residual = dot(hpsi - dot(psi, full, last), mix, last)
    return residual, projected


def body(psi, vpsi, kinetic, mixing):
    n_grow = lax.axis_size("grow")
    n_gcol = lax.axis_size("gcol")
    rows, nb = psi.shape
    fits = (n_grow == 2 * 2 and n_gcol % 2 == 0 and nb % (8 * n_grow * n_gcol) == 0
            and (nb // n_gcol) % 128 == 0 and (nb // n_grow) % 256 == 0 and rows % 512 == 0)
    return (body_kernel if fits else body_plain)(psi, vpsi, kinetic, mixing)


def solution(mesh):
    return jax.shard_map(
        body,
        mesh=mesh,
        in_specs=(
            P(("grow", "gcol"), None),
            P(("grow", "gcol"), None),
            P(("grow", "gcol")),
            P("grow", "gcol"),
        ),
        out_specs=(P(("grow", "gcol"), None), P("grow", "gcol")),
        check_vma=False,
    )
```
